32 devices in a mesh: dp: 8 (over z, x), vocab: 4 (over y, core).
Axes of the slice: x: 2, y: 2, z: 4, core: 2. Of those that a mesh axis runs over, the one named last changes fastest.
Arguments:
- hidden_states: bfloat16 [1024, 3584], P('dp'), may hold values from -40 to 40
- head_weight: bfloat16 [3584, 98304], P(None, ('dp', 'vocab')), as said below
- target_ids: int32 [1024], replicated, may hold values from 0 to 98303
- seq_lengths: int32 [64], P('dp'), may hold values from 1 to 16
- domain_labels: int32 [64], P('dp'), may hold values from 0 to 21
- domain_weights: float32 [22], replicated, may hold values from 0.5 to 4
Outputs:
- token_loss: float32 [1024], P('dp')
- new_weights: float32 [22], replicated
The draws below stay inside these ranges and needn't reach their ends.
Inputs may be any that keep to these rules, and one draw needn't show every extreme that they name: `head_weight`: every entry lies within 6 / sqrt(3584) of zero.
All inputs are finite; a program needn't handle non-finite values.
Results may differ from the reference program's by a relative error of at most 0.0003.
Values may be sent and summed in bfloat16 or wider, within the bound.
A program may use at most 128 MiB of HBM per device.

```python
import math
import jax
import jax.numpy as jnp
import numpy as np
from jax import lax

D = 3584
VOCAB = 98304
SEQ_LEN = 16
DOMAINS = 22
SEQS = 64
TOKENS = 1024
N_DP = 8


def weight_table(key):
    base = jax.random.normal(jax.random.fold_in(key, 11), (D, VOCAB), jnp.float32)
    return jnp.clip(base, -6.0, 6.0) / math.sqrt(D)


def draw_head_weight(key, part):
    return weight_table(key).astype(jnp.bfloat16)


def draw_hidden_states(key, part):
    base = jax.random.normal(jax.random.fold_in(key, 31), (TOKENS, D), jnp.float32)
    return jnp.clip(3.0 * base, -18.0, 18.0).astype(jnp.bfloat16)


def plant(entries, own_key, least, high):
    dims = entries.shape
    spot = [jax.random.randint(jax.random.fold_in(own_key, axis), (), 0, dims[axis]) for axis in range(len(dims))]
    entries = entries.at[tuple(spot)].set(least)
    longest = dims.index(max(dims))
    spot[longest] = (spot[longest] + 1) % dims[longest]
    return entries.at[tuple(spot)].set(high)


def cumulative_ranks(number_of, lean):
    portions = [(1 << 20) // math.isqrt(standing ** lean) + 1 for standing in range(1, number_of + 1)]
    deviation = 1 + sum(portions) // (1 << 30)
    return np.cumsum(np.array([max(1, weight // deviation) for weight in portions]))


def skewed_ids(stream_key, extent, count, lean):
    grid = cumulative_ranks(count, lean)
    lot = jax.random.randint(jax.random.fold_in(stream_key, 1), extent, 0, int(grid[count - 1]))
    grade = jnp.searchsorted(jnp.asarray(grid, jnp.int32), lot, side="right")
    return jax.random.permutation(jax.random.fold_in(stream_key, 2), count)[grade].astype(jnp.int32)


def setup_inputs(seed: int = 0) -> dict:
    seeds = jax.random.split(jax.random.key(seed), 7)
    hidden_states = draw_hidden_states(jax.random.fold_in(seeds[6], 71), 0)
    head_weight = draw_head_weight(jax.random.fold_in(seeds[6], 71), 0)
    target_ids = plant(jax.random.randint(seeds[2], (TOKENS,), 0, VOCAB), jax.random.fold_in(seeds[2], 1), 0, VOCAB - 1).astype(jnp.int32)
    seq_lengths = plant(jax.random.randint(seeds[3], (SEQS,), 1, SEQ_LEN + 1), jax.random.fold_in(seeds[3], 1), 1, SEQ_LEN).astype(jnp.int32)
    domain_labels = plant(skewed_ids(seeds[4], (SEQS,), DOMAINS, 2), jax.random.fold_in(seeds[4], 3), 0, DOMAINS - 1).astype(jnp.int32)
    domain_weights = jnp.clip(jnp.exp(jax.random.uniform(seeds[5], (DOMAINS,), jnp.float32, math.log(0.5), math.log(4.0))), 0.5, 4.0)
    return dict(hidden_states=hidden_states, head_weight=head_weight, target_ids=target_ids, seq_lengths=seq_lengths, domain_labels=domain_labels, domain_weights=domain_weights)


explore_share = 0.01
step_rate = 0.002


def reference(hidden_states, head_weight, target_ids, seq_lengths, domain_labels, domain_weights):
    def block_loss(block):
        block_rows, targets = block
        logits = jnp.dot(block_rows, head_weight, preferred_element_type=jnp.float32)
        row_peak = jnp.max(logits, axis=1)
        mass_sum = jnp.sum(jnp.exp(logits - row_peak[:, None]), axis=1)
        picked = jnp.take_along_axis(logits, targets[:, None], axis=1)[:, 0]
        return jnp.log(mass_sum) + row_peak - picked

    blocks = (hidden_states.reshape(N_DP, -1, D), target_ids.reshape(N_DP, -1))
    raw_loss = lax.map(block_loss, blocks).reshape(-1)
    positions = jnp.arange(TOKENS) % SEQ_LEN
    valid = positions < jnp.repeat(seq_lengths, SEQ_LEN)
    token_loss = jnp.where(valid, raw_loss, 0.0)
    seq_loss = jnp.sum(token_loss.reshape(-1, SEQ_LEN), axis=1)
    seq_tokens = seq_lengths.astype(jnp.float32)
    domain_hot = (domain_labels[:, None] == jnp.arange(DOMAINS)[None, :]).astype(jnp.float32)
    domain_loss = jnp.sum(domain_hot * seq_loss[:, None], axis=0)
    domain_count = jnp.sum(domain_hot * seq_tokens[:, None], axis=0)
    probability = (1.0 - DOMAINS * explore_share) * domain_weights / jnp.sum(domain_weights) + explore_share
    reward = domain_loss / jnp.maximum(domain_count, 1.0) / probability
    raised = domain_weights * jnp.exp(step_rate * reward)
    new_weights = DOMAINS * raised / jnp.sum(raised)
    return token_loss, new_weights
```

```python
import functools
import math

import jax
import jax.numpy as jnp
from jax import lax
from jax.experimental import pallas as pl
from jax.experimental.pallas import tpu as pltpu
from jax.sharding import PartitionSpec as P

SEQ_LEN = 16
DOMAINS = 22
LANES = 128
DOM_PAD = 24
CORES = 2

explore_share = 0.01
step_rate = 0.002


def nearest(p, i, n):
    if n == 2:
        return p if i == 0 else 1 - p
    m = jnp.minimum(p, n - 1 - p)
    k = (i + 1) // 2
    both = jnp.where(i % 2 == 1, p + k, p - k)
    far = i - m
    one = jnp.where(p + p <= n - 1, p + far, p - far)
    return jnp.where(i <= 2 * m, both, one)


def kernel(Z, X, Y, tok, cols, TN,
           hid_ref, w_ref, tgt_ref, len_ref, lab_ref, dw_ref,
           loss_ref, new_ref,
           buf, w_buf, m_ref, s_ref, p_ref, stat_out, stat_in, dom_out, dom_in,
           own_sem, w_sem, recv_sem, send_sem, st_send, st_recv, dm_send, dm_recv):
    nv = Y * CORES
    dp = Z * X
    ndev = dp * nv
    T = cols // TN
    M = X * tok
    pr = tok // nv
    me = lax.axis_index("dp")
    v = lax.axis_index("vocab")
    z, x = me // X, me % X
    y, c = v // CORES, v % CORES

    own_copy = pltpu.make_async_copy(hid_ref, buf.at[pl.ds(me * tok, tok)], own_sem)
    own_copy.start()

    def w_copy(j):
        return pltpu.make_async_copy(
            w_ref.at[:, pl.ds(pl.multiple_of(j * TN, TN), TN)], w_buf.at[j], w_sem.at[j]
        )

    for j in range(T):
        w_copy(j).start()

    def remote(kind, zs, xs, ys, cs, to):
        piece = ((zs * X + xs) * Y + ys) * CORES + cs
        rows = buf.at[pl.ds(pl.multiple_of(piece * pr, pr), pr)]
        return pltpu.make_async_remote_copy(
            src_ref=rows, dst_ref=rows,
            send_sem=send_sem.at[kind, piece], recv_sem=recv_sem.at[piece],
            device_id=to, device_id_type=pl.DeviceIdType.MESH,
        )

    def push(drain, cond, *what):
        def go():
            r = remote(*what)
            if drain:
                r.wait_send()
            else:
                r.start()
        if cond is None:
            go()
        else:
            pl.when(cond)(go)

    def dev(z_, x_, y_, c_):
        return (z_ * X + x_, y_ * CORES + c_)

    def arrive(drain, zs, xs, ys, cs):
        if not drain:
            remote(0, zs, xs, ys, cs, dev(z, x, y, 1 - c)).wait_recv()

    def line(drain, kind, n, pos, src, at, piece):
        up, down = pos + 1 < n, pos > 0
        if src is not None:
            if n == 2:
                return
            up, down = up & (src < pos), down & (src > pos)
        if n == 2:
            push(drain, None, kind, *piece, at(1 - pos))
            return
        push(drain, up, kind, *piece, at(pos + 1))
        push(drain, down, kind + 1, *piece, at(pos - 1))

    def send_z(drain, src, piece):
        line(drain, 1, Z, z, src, lambda q: dev(q, x, y, c), piece)

    def send_x(drain, src, piece):
        line(drain, 3, X, x, src, lambda q: dev(z, q, y, c), piece)

    def send_y(drain, src, piece):
        line(drain, 5, Y, y, src, lambda q: dev(z, x, q, c), piece)

    def send_c(drain, piece):
        push(drain, None, 0, *piece, dev(z, x, y, 1 - c))

    def y_first(i):
        return i == 0 or i == Z - 1

    def begin(drain):
        send_z(drain, None, (z, x, y, c))
        for k in range(Y):
            send_x(drain, None, (z, x, k, c))

    def z_step(drain, i):
        zs = nearest(z, i, Z)
        piece = (zs, x, y, c)
        arrive(drain, *piece)
        send_z(drain, zs, piece)
        send_y(drain, None, piece)
        send_x(drain, None, piece)
        send_c(drain, piece)

    def first_step(drain, i):
        zs = nearest(z, i, Z)
        if y_first(i):
            for t in range(1, Y):
                ys = nearest(y, t, Y)
                piece = (zs, x, ys, c)
                arrive(drain, *piece)
                send_y(drain, ys, piece)
                send_x(drain, None, piece)
                send_c(drain, piece)
        else:
            for t in range(1, X):
                xs = nearest(x, t, X)
                piece = (zs, xs, y, c)
                arrive(drain, *piece)
                send_x(drain, xs, piece)
                send_y(drain, None, piece)
                send_c(drain, piece)

    def second_step(drain, i):
        zs = nearest(z, i, Z)
        if y_first(i):
            for t in range(1, X):
                xs = nearest(x, t, X)
                for s in range(Y):
                    ys = nearest(y, s, Y)
                    piece = (zs, xs, ys, c)
                    arrive(drain, *piece)
                    send_x(drain, xs, piece)
                    send_c(drain, piece)
        else:
            for t in range(1, Y):
                ys = nearest(y, t, Y)
                for s in range(X):
                    xs = nearest(x, s, X)
                    piece = (zs, xs, ys, c)
                    arrive(drain, *piece)
                    send_y(drain, ys, piece)
                    send_c(drain, piece)

    def core_step(drain, i):
        zs = nearest(z, i, Z)
        for t in range(1 if i == 0 else 0, X):
            xs = nearest(x, t, X)
            for ys in range(Y):
                arrive(drain, zs, xs, ys, 1 - c)

    events = []
    for u in range(Z - 1):
        at = lambda twelfth: min(T - 1, twelfth * T // 12)
        if u == 0:
            if Z > 2:
                events.append((0, at(1), z_step, 2))
            events.append((0, at(5), first_step, 1))
            if Z > 3:
                events.append((0, at(8), z_step, 3))
            if Z > 2:
                events.append((0, at(11), first_step, 2))
        else:
            if u + 3 < Z:
                events.append((u, at(2), z_step, u + 3))
            if u + 2 < Z:
                events.append((u, at(3), first_step, u + 2))
        events.append((u, T - 1, second_step, u + 1))
        events.append((u, T - 1, core_step, u + 1))
    tile_events = [e for e in events if e[2] in (z_step, first_step)]
    end_events = [e for e in events if e[2] in (second_step, core_step)]

    own_copy.wait()
    begin(False)
    if Z > 1:
        z_step(False, 1)
    second_step(False, 0)
    core_step(False, 0)

    lane = lax.broadcasted_iota(jnp.int32, (M, LANES), 1)
    col_start = (me * nv + v) * cols

    def plane(u, _):
        zs = z if Z == 1 else nearest(z, u, Z) if Z != 2 else jnp.where(u == 0, z, 1 - z)
        r0 = pl.multiple_of(zs * M, M)
        m_ref[...] = jnp.full((M, LANES), -1e30, jnp.float32)
        s_ref[...] = jnp.zeros((M, LANES), jnp.float32)
        p_ref[...] = jnp.zeros((M, LANES), jnp.float32)

        def tile(j, _):
            for (eu, ej, fn, i) in tile_events:
                pl.when((u == eu) & (j == ej))(functools.partial(fn, False, i))

            @pl.when(u == 0)
            def _():
                w_copy(j).wait()

            logits = jnp.dot(buf[pl.ds(r0, M), :], w_buf[j], preferred_element_type=jnp.float32)
            off = tgt_ref[pl.ds(r0, M), :] - (col_start + j * TN) - lane
            m_old = m_ref[...]
            parts = [logits[:, g * LANES:(g + 1) * LANES] for g in range(TN // LANES)]
            m_new = m_old
            for a in parts:
                m_new = jnp.maximum(m_new, a)
            s = s_ref[...] * jnp.exp(m_old - m_new)
            pk = p_ref[...]
            for g, a in enumerate(parts):
                s = s + jnp.exp(a - m_new)
                pk = pk + jnp.where(off == g * LANES, a, 0.0)
            m_ref[...] = m_new
            s_ref[...] = s
            p_ref[...] = pk
            return 0

        lax.fori_loop(0, T, tile, 0)

        row_m = jnp.max(m_ref[...], axis=1, keepdims=True)
        row_s = jnp.sum(s_ref[...] * jnp.exp(m_ref[...] - row_m), axis=1, keepdims=True)
        row_p = jnp.sum(p_ref[...], axis=1, keepdims=True)
        packed = jnp.where(lane == 0, row_m, jnp.where(lane == 1, row_s, jnp.where(lane == 2, row_p, 0.0)))
        for xs in range(X):
            stat_out[zs * X + xs] = jnp.transpose(packed[xs * tok:(xs + 1) * tok])[:8]
        for xs in range(X):
            d = zs * X + xs

            @pl.when(d == me)
            def _():
                stat_in[me * nv + v] = stat_out[me]

            for k in range(nv):
                @pl.when((d != me) | (v != k))
                def _():
                    pltpu.make_async_remote_copy(
                        src_ref=stat_out.at[d], dst_ref=stat_in.at[me * nv + v],
                        send_sem=st_send, recv_sem=st_recv,
                        device_id=(d, k), device_id_type=pl.DeviceIdType.MESH,
                    ).start()
        for (eu, ej, fn, i) in end_events:
            pl.when(u == eu)(functools.partial(fn, False, i))
        return 0

    lax.fori_loop(0, Z, plane, 0)

    others = stat_in.at[pl.ds(0, ndev - 1)]
    pltpu.make_async_copy(others, others, st_recv).wait()
    ms = stat_in[:, 0, :]
    peak = jnp.max(ms, axis=0, keepdims=True)
    mass = jnp.sum(stat_in[:, 1, :] * jnp.exp(ms - peak), axis=0, keepdims=True)
    pick = jnp.sum(stat_in[:, 2, :], axis=0, keepdims=True)
    position = lax.broadcasted_iota(jnp.int32, (1, tok), 1) % SEQ_LEN
    valid = position < len_ref[...]
    loss = jnp.where(valid, jnp.log(mass) + peak - pick, 0.0)
    loss_ref[...] = loss
    dom = lax.broadcasted_iota(jnp.int32, (DOM_PAD, tok), 0)
    hot = dom == lab_ref[...]
    d_loss = jnp.sum(jnp.where(hot, loss, 0.0), axis=1, keepdims=True)
    d_count = jnp.sum(jnp.where(hot & valid, 1.0, 0.0), axis=1, keepdims=True)
    dlane = lax.broadcasted_iota(jnp.int32, (DOM_PAD, LANES), 1)
    dom_out[...] = jnp.where(dlane == 0, d_loss, jnp.where(dlane == 1, d_count, 0.0))
    dom_in[me] = dom_out[...]
    for k in range(1, dp):
        pltpu.make_async_remote_copy(
            src_ref=dom_out, dst_ref=dom_in.at[me],
            send_sem=dm_send, recv_sem=dm_recv,
            device_id=((me + k) % dp, v), device_id_type=pl.DeviceIdType.MESH,
        ).start()

    begin(True)
    if Z > 1:
        z_step(True, 1)
    second_step(True, 0)
    for (eu, ej, fn, i) in events:
        fn(True, i)
    pltpu.make_async_copy(others, others, st_send).wait()

    rest = dom_in.at[pl.ds(0, dp - 1)]
    pltpu.make_async_copy(rest, rest, dm_recv).wait()
    total = jnp.sum(dom_in[...], axis=0)
    dom_loss = jnp.sum(jnp.where(dlane == 0, total, 0.0), axis=1, keepdims=True)
    dom_count = jnp.sum(jnp.where(dlane == 1, total, 0.0), axis=1, keepdims=True)
    live = lax.broadcasted_iota(jnp.int32, (DOM_PAD, LANES), 0) < DOMAINS
    weights = jnp.where(live, dw_ref[...], 0.0)
    probability = (1.0 - DOMAINS * explore_share) * weights / jnp.sum(
        weights, axis=0, keepdims=True) + explore_share
    reward = dom_loss / jnp.maximum(dom_count, 1.0) / probability
    raised = jnp.where(live, weights * jnp.exp(step_rate * reward), 0.0)
    new_ref[...] = DOMAINS * raised / jnp.sum(raised, axis=0, keepdims=True)
    pltpu.make_async_copy(rest, rest, dm_send).wait()


def body(hidden_states, head_weight, target_ids, seq_lengths, domain_labels, domain_weights):
    tok, width = hidden_states.shape
    cols = head_weight.shape[1]
    dp = lax.axis_size("dp")
    nv = lax.axis_size("vocab")
    X = math.isqrt(dp // 2)
    Z = dp // X
    Y = nv // CORES
    tokens = dp * tok
    TN = 2 * LANES if cols % (2 * LANES) == 0 else LANES
    T = cols // TN
    M = X * tok
    tgt = jnp.broadcast_to(target_ids[:, None], (tokens, LANES))
    lens = jnp.repeat(seq_lengths, SEQ_LEN)[None, :]
    labs = jnp.repeat(domain_labels, SEQ_LEN)[None, :]
    dw = jnp.broadcast_to(
        jnp.concatenate([domain_weights, jnp.ones((DOM_PAD - DOMAINS,), jnp.float32)])[:, None],
        (DOM_PAD, LANES),
    )
    hbm = pl.BlockSpec(memory_space=pl.ANY)
    vmem = pl.BlockSpec(memory_space=pltpu.VMEM)
    f32 = jnp.float32
    dma = pltpu.SemaphoreType.DMA
    loss, new = pl.pallas_call(
        functools.partial(kernel, Z, X, Y, tok, cols, TN),
        out_shape=(jax.ShapeDtypeStruct((1, tok), f32), jax.ShapeDtypeStruct((DOM_PAD, LANES), f32)),
        in_specs=[hbm, hbm, vmem, vmem, vmem, vmem],
        out_specs=(vmem, vmem),
        scratch_shapes=[
            pltpu.VMEM((tokens, width), hidden_states.dtype),
            pltpu.VMEM((T, width, TN), head_weight.dtype),
            pltpu.VMEM((M, LANES), f32),
            pltpu.VMEM((M, LANES), f32),
            pltpu.VMEM((M, LANES), f32),
            pltpu.VMEM((dp, 8, tok), f32),
            pltpu.VMEM((dp * nv, 8, tok), f32),
            pltpu.VMEM((DOM_PAD, LANES), f32),
            pltpu.VMEM((dp, DOM_PAD, LANES), f32),
            dma(()),
            dma((T,)),
            dma((dp * nv,)),
            dma((7, dp * nv)),
            dma(()), dma(()), dma(()), dma(()),
        ],
        compiler_params=pltpu.CompilerParams(has_side_effects=True, vmem_limit_bytes=60 * 2**20),
    )(hidden_states, head_weight, tgt, lens, labs, dw)
    return loss[0], new[:DOMAINS, 0]


def solution(mesh):
    placed = (P("dp", None), P(None, ("dp", "vocab")), P(), P("dp"), P("dp"), P())
    return jax.shard_map(
        body, mesh=mesh, in_specs=placed, out_specs=(P("dp"), P()), check_vma=False
    )
```

```python
import functools
import math

import jax
import jax.numpy as jnp
from jax import lax
from jax.experimental import pallas as pl
from jax.experimental.pallas import tpu as pltpu
from jax.sharding import PartitionSpec as P

SEQ_LEN = 16
DOMAINS = 22
LANES = 128
DOM_PAD = 24
CORES = 2

explore_share = 0.01
step_rate = 0.002


def nearest(p, i, n):
    if n == 2:
        return p if i == 0 else 1 - p
    m = jnp.minimum(p, n - 1 - p)
    k = (i + 1) // 2
    both = jnp.where(i % 2 == 1, p + k, p - k)
    far = i - m
    one = jnp.where(p + p <= n - 1, p + far, p - far)
    return jnp.where(i <= 2 * m, both, one)


def kernel(Z, X, Y, tok, cols, TN,
           hid_ref, w_ref, tgt_ref, len_ref, lab_ref, dw_ref,
           loss_ref, new_ref,
           buf, w_buf, m_ref, s_ref, p_ref, stat_out, stat_in, dom_out, dom_in,
           own_sem, w_sem, recv_sem, send_sem, st_send, st_recv, dm_send, dm_recv):
    nv = Y * CORES
    dp = Z * X
    ndev = dp * nv
    T = cols // TN
    M = X * tok
    pr = tok // nv
    me = lax.axis_index("dp")
    v = lax.axis_index("vocab")
    z, x = me // X, me % X
    y, c = v // CORES, v % CORES

    own_copy = pltpu.make_async_copy(hid_ref, buf.at[pl.ds(me * tok, tok)], own_sem)
    own_copy.start()

    def w_copy(j):
        return pltpu.make_async_copy(
            w_ref.at[:, pl.ds(pl.multiple_of(j * TN, TN), TN)], w_buf.at[j], w_sem.at[j]
        )

    for j in range(T):
        w_copy(j).start()

    def remote(kind, zs, xs, ys, cs, to):
        piece = ((zs * X + xs) * Y + ys) * CORES + cs
        rows = buf.at[pl.ds(pl.multiple_of(piece * pr, pr), pr)]
        return pltpu.make_async_remote_copy(
            src_ref=rows, dst_ref=rows,
            send_sem=send_sem.at[kind, piece], recv_sem=recv_sem.at[piece],
            device_id=to, device_id_type=pl.DeviceIdType.MESH,
        )

    def push(drain, cond, *what):
        def go():
            r = remote(*what)
            if drain:
                r.wait_send()
            else:
                r.start()
        if cond is None:
            go()
        else:
            pl.when(cond)(go)

    def dev(z_, x_, y_, c_):
        return (z_ * X + x_, y_ * CORES + c_)

    def arrive(drain, zs, xs, ys, cs):
        if not drain:
            remote(0, zs, xs, ys, cs, dev(z, x, y, 1 - c)).wait_recv()

    def line(drain, kind, n, pos, src, at, piece):
        up, down = pos + 1 < n, pos > 0
        if src is not None:
            if n == 2:
                return
            up, down = up & (src < pos), down & (src > pos)
        if n == 2:
            push(drain, None, kind, *piece, at(1 - pos))
            return
        push(drain, up, kind, *piece, at(pos + 1))
        push(drain, down, kind + 1, *piece, at(pos - 1))

    def send_z(drain, src, piece):
        line(drain, 1, Z, z, src, lambda q: dev(q, x, y, c), piece)

    def send_x(drain, src, piece):
        line(drain, 3, X, x, src, lambda q: dev(z, q, y, c), piece)

    def send_y(drain, src, piece):
        line(drain, 5, Y, y, src, lambda q: dev(z, x, q, c), piece)

    def send_c(drain, piece):
        push(drain, None, 0, *piece, dev(z, x, y, 1 - c))

    def y_first(i):
        return i == 0 or i == Z - 1

    def begin(drain):
        send_z(drain, None, (z, x, y, c))
        for k in range(Y):
            send_x(drain, None, (z, x, k, c))

    def z_step(drain, i):
        zs = nearest(z, i, Z)
        piece = (zs, x, y, c)
        arrive(drain, *piece)
        send_z(drain, zs, piece)
        send_y(drain, None, piece)
        send_x(drain, None, piece)
        send_c(drain, piece)

    def first_step(drain, i):
        zs = nearest(z, i, Z)
        if y_first(i):
            for t in range(1, Y):
                ys = nearest(y, t, Y)
                piece = (zs, x, ys, c)
                arrive(drain, *piece)
                send_y(drain, ys, piece)
                send_x(drain, None, piece)
                send_c(drain, piece)
        else:
            for t in range(1, X):
                xs = nearest(x, t, X)
                piece = (zs, xs, y, c)
                arrive(drain, *piece)
                send_x(drain, xs, piece)
                send_y(drain, None, piece)
                send_c(drain, piece)

    def second_step(drain, i):
        zs = nearest(z, i, Z)
        if y_first(i):
            for t in range(1, X):
                xs = nearest(x, t, X)
                for s in range(Y):
                    ys = nearest(y, s, Y)
                    piece = (zs, xs, ys, c)
                    arrive(drain, *piece)
                    send_x(drain, xs, piece)
                    send_c(drain, piece)
        else:
            for t in range(1, Y):
                ys = nearest(y, t, Y)
                for s in range(X):
                    xs = nearest(x, s, X)
                    piece = (zs, xs, ys, c)
                    arrive(drain, *piece)
                    send_y(drain, ys, piece)
                    send_c(drain, piece)

    def core_step(drain, i):
        zs = nearest(z, i, Z)
        for t in range(1 if i == 0 else 0, X):
            xs = nearest(x, t, X)
            for ys in range(Y):
                arrive(drain, zs, xs, ys, 1 - c)

    events = []
    for u in range(Z - 1):
        at = lambda twelfth: min(T - 1, twelfth * T // 12)
        if u == 0:
            events.append((0, at(0), first_step, 1))
            if Z > 3:
                events.append((0, at(2), z_step, 3))
            if Z > 2:
                events.append((0, at(6), first_step, 2))
        else:
            if u + 3 < Z:
                events.append((u, at(2), z_step, u + 3))
            if u + 2 < Z:
                events.append((u, at(3), first_step, u + 2))
        events.append((u, T - 1, second_step, u + 1))
        events.append((u, T - 1, core_step, u + 1))
    tile_events = [e for e in events if e[2] in (z_step, first_step)]
    end_events = [e for e in events if e[2] in (second_step, core_step)]

    own_copy.wait()
    begin(False)
    if Z > 1:
        z_step(False, 1)
    if Z > 2:
        z_step(False, 2)
    second_step(False, 0)
    core_step(False, 0)

    lane = lax.broadcasted_iota(jnp.int32, (M, LANES), 1)
    col_start = (me * nv + v) * cols

    def plane(u, _):
        zs = z if Z == 1 else nearest(z, u, Z) if Z != 2 else jnp.where(u == 0, z, 1 - z)
        r0 = pl.multiple_of(zs * M, M)
        m_ref[...] = jnp.full((M, LANES), -1e30, jnp.float32)
        s_ref[...] = jnp.zeros((M, LANES), jnp.float32)
        p_ref[...] = jnp.zeros((M, LANES), jnp.float32)

        def tile(j, _):
            for (eu, ej, fn, i) in tile_events:
                pl.when((u == eu) & (j == ej))(functools.partial(fn, False, i))

            @pl.when(u == 0)
            def _():
                w_copy(j).wait()

            logits = jnp.dot(buf[pl.ds(r0, M), :], w_buf[j], preferred_element_type=jnp.float32)
            off = tgt_ref[pl.ds(r0, M), :] - (col_start + j * TN) - lane
            m_old = m_ref[...]
            parts = [logits[:, g * LANES:(g + 1) * LANES] for g in range(TN // LANES)]
            m_new = m_old
            for a in parts:
                m_new = jnp.maximum(m_new, a)
            s = s_ref[...] * jnp.exp(m_old - m_new)
            pk = p_ref[...]
            for g, a in enumerate(parts):
                s = s + jnp.exp(a - m_new)
                pk = pk + jnp.where(off == g * LANES, a, 0.0)
            m_ref[...] = m_new
            s_ref[...] = s
            p_ref[...] = pk
            return 0

        lax.fori_loop(0, T, tile, 0)

        row_m = jnp.max(m_ref[...], axis=1, keepdims=True)
        row_s = jnp.sum(s_ref[...] * jnp.exp(m_ref[...] - row_m), axis=1, keepdims=True)
        row_p = jnp.sum(p_ref[...], axis=1, keepdims=True)
        packed = jnp.where(lane == 0, row_m, jnp.where(lane == 1, row_s, jnp.where(lane == 2, row_p, 0.0)))
        for xs in range(X):
            stat_out[zs * X + xs] = jnp.transpose(packed[xs * tok:(xs + 1) * tok])[:8]
        for xs in range(X):
            d = zs * X + xs

            @pl.when(d == me)
            def _():
                stat_in[me * nv + v] = stat_out[me]

            for k in range(nv):
                @pl.when((d != me) | (v != k))
                def _():
                    pltpu.make_async_remote_copy(
                        src_ref=stat_out.at[d], dst_ref=stat_in.at[me * nv + v],
                        send_sem=st_send, recv_sem=st_recv,
                        device_id=(d, k), device_id_type=pl.DeviceIdType.MESH,
                    ).start()
        for (eu, ej, fn, i) in end_events:
            pl.when(u == eu)(functools.partial(fn, False, i))
        return 0

    lax.fori_loop(0, Z, plane, 0)

    others = stat_in.at[pl.ds(0, ndev - 1)]
    pltpu.make_async_copy(others, others, st_recv).wait()
    ms = stat_in[:, 0, :]
    peak = jnp.max(ms, axis=0, keepdims=True)
    mass = jnp.sum(stat_in[:, 1, :] * jnp.exp(ms - peak), axis=0, keepdims=True)
    pick = jnp.sum(stat_in[:, 2, :], axis=0, keepdims=True)
    position = lax.broadcasted_iota(jnp.int32, (1, tok), 1) % SEQ_LEN
    valid = position < len_ref[...]
    loss = jnp.where(valid, jnp.log(mass) + peak - pick, 0.0)
    loss_ref[...] = loss
    dom = lax.broadcasted_iota(jnp.int32, (DOM_PAD, tok), 0)
    hot = dom == lab_ref[...]
    d_loss = jnp.sum(jnp.where(hot, loss, 0.0), axis=1, keepdims=True)
    d_count = jnp.sum(jnp.where(hot & valid, 1.0, 0.0), axis=1, keepdims=True)
    dlane = lax.broadcasted_iota(jnp.int32, (DOM_PAD, LANES), 1)
    dom_out[...] = jnp.where(dlane == 0, d_loss, jnp.where(dlane == 1, d_count, 0.0))
    dom_in[me] = dom_out[...]
    for k in range(1, dp):
        pltpu.make_async_remote_copy(
            src_ref=dom_out, dst_ref=dom_in.at[me],
            send_sem=dm_send, recv_sem=dm_recv,
            device_id=((me + k) % dp, v), device_id_type=pl.DeviceIdType.MESH,
        ).start()

    begin(True)
    if Z > 1:
        z_step(True, 1)
    if Z > 2:
        z_step(True, 2)
    second_step(True, 0)
    for (eu, ej, fn, i) in events:
        fn(True, i)
    pltpu.make_async_copy(others, others, st_send).wait()

    rest = dom_in.at[pl.ds(0, dp - 1)]
    pltpu.make_async_copy(rest, rest, dm_recv).wait()
    total = jnp.sum(dom_in[...], axis=0)
    dom_loss = jnp.sum(jnp.where(dlane == 0, total, 0.0), axis=1, keepdims=True)
    dom_count = jnp.sum(jnp.where(dlane == 1, total, 0.0), axis=1, keepdims=True)
    live = lax.broadcasted_iota(jnp.int32, (DOM_PAD, LANES), 0) < DOMAINS
    weights = jnp.where(live, dw_ref[...], 0.0)
    probability = (1.0 - DOMAINS * explore_share) * weights / jnp.sum(
        weights, axis=0, keepdims=True) + explore_share
    reward = dom_loss / jnp.maximum(dom_count, 1.0) / probability
    raised = jnp.where(live, weights * jnp.exp(step_rate * reward), 0.0)
    new_ref[...] = DOMAINS * raised / jnp.sum(raised, axis=0, keepdims=True)
    pltpu.make_async_copy(rest, rest, dm_send).wait()


def body(hidden_states, head_weight, target_ids, seq_lengths, domain_labels, domain_weights):
    tok, width = hidden_states.shape
    cols = head_weight.shape[1]
    dp = lax.axis_size("dp")
    nv = lax.axis_size("vocab")
    X = math.isqrt(dp // 2)
    Z = dp // X
    Y = nv // CORES
    tokens = dp * tok
    TN = 2 * LANES if cols % (2 * LANES) == 0 else LANES
    T = cols // TN
    M = X * tok
    tgt = jnp.broadcast_to(target_ids[:, None], (tokens, LANES))
    lens = jnp.repeat(seq_lengths, SEQ_LEN)[None, :]
    labs = jnp.repeat(domain_labels, SEQ_LEN)[None, :]
    dw = jnp.broadcast_to(
        jnp.concatenate([domain_weights, jnp.ones((DOM_PAD - DOMAINS,), jnp.float32)])[:, None],
        (DOM_PAD, LANES),
    )
    hbm = pl.BlockSpec(memory_space=pl.ANY)
    vmem = pl.BlockSpec(memory_space=pltpu.VMEM)
    f32 = jnp.float32
    dma = pltpu.SemaphoreType.DMA
    loss, new = pl.pallas_call(
        functools.partial(kernel, Z, X, Y, tok, cols, TN),
        out_shape=(jax.ShapeDtypeStruct((1, tok), f32), jax.ShapeDtypeStruct((DOM_PAD, LANES), f32)),
        in_specs=[hbm, hbm, vmem, vmem, vmem, vmem],
        out_specs=(vmem, vmem),
        scratch_shapes=[
            pltpu.VMEM((tokens, width), hidden_states.dtype),
            pltpu.VMEM((T, width, TN), head_weight.dtype),
            pltpu.VMEM((M, LANES), f32),
            pltpu.VMEM((M, LANES), f32),
            pltpu.VMEM((M, LANES), f32),
            pltpu.VMEM((dp, 8, tok), f32),
            pltpu.VMEM((dp * nv, 8, tok), f32),
            pltpu.VMEM((DOM_PAD, LANES), f32),
            pltpu.VMEM((dp, DOM_PAD, LANES), f32),
            dma(()),
            dma((T,)),
            dma((dp * nv,)),
            dma((7, dp * nv)),
            dma(()), dma(()), dma(()), dma(()),
        ],
        compiler_params=pltpu.CompilerParams(has_side_effects=True, vmem_limit_bytes=60 * 2**20),
    )(hidden_states, head_weight, tgt, lens, labs, dw)
    return loss[0], new[:DOMAINS, 0]


def solution(mesh):
    placed = (P("dp", None), P(None, ("dp", "vocab")), P(), P("dp"), P("dp"), P())
    return jax.shard_map(
        body, mesh=mesh, in_specs=placed, out_specs=(P("dp"), P()), check_vma=False
    )
```
